1024 devices in a mesh: gz: 32 (over z_hi, y), gy: 4 (over x), gx: 8 (over z_lo, core).
Axes of the slice: x: 4, y: 8, z: 16 (z_hi: 4, z_lo: 4; z = z_hi * 4 + z_lo), core: 2. Of those that a mesh axis runs over, the one named last changes fastest.
Arguments:
- positions: float32 [3, 8, 8, 256, 128], P(None, 'gx', 'gy', 'gz'), may hold values from 0 to 1
- counts: int32 [8, 8, 256], P('gx', 'gy', 'gz'), may hold values from 104 to 128
Outputs:
- energy: float32 [8, 8, 256, 128], P('gx', 'gy', 'gz')
- forces: float32 [3, 8, 8, 256, 128], P(None, 'gx', 'gy', 'gz')
The draws below stay inside these ranges and needn't reach their ends.
Inputs may be any that keep to these rules, and one draw needn't show every extreme that they name: `counts`: slot k of a cell holds an atom exactly when k < its count; positions of other slots are not used.
All inputs are finite; a program needn't handle non-finite values.
Results may differ from the reference program's by a relative error of at most 0.0003.
Values sent between devices are 32-bit elements; how exact they have to be, the bound alone decides.
No kernel may reach another device: no remote copies, remote signals or barrier semaphores. Data moves between devices by JAX's collectives and lax.ppermute only.
A program may use at most 32 MiB of HBM per device.

```python
import jax
import jax.numpy as jnp
from jax import lax

S = 128
NX = 8
NY = 8
NZ = 256


def touch_ends(result, own_key, smallest, top_value):
    dims = result.shape
    index_at = [jax.random.randint(jax.random.fold_in(own_key, axis), (), 0, dims[axis]) for axis in range(len(dims))]
    result = result.at[tuple(index_at)].set(smallest)
    longest = dims.index(max(dims))
    index_at[longest] = (index_at[longest] + 1) % dims[longest]
    return result.at[tuple(index_at)].set(top_value)


def block_scale(key, extent, shards, least, high):
    level = 1.0
    for dim, blocks in shards:
        steps = jax.random.uniform(jax.random.fold_in(jax.random.fold_in(key, 6), dim), (blocks,), jnp.float32, least / len(shards), high / len(shards))
        level = level * jnp.repeat(jnp.exp(steps), extent[dim] // blocks).reshape((-1,) + (1,) * (len(extent) - 1 - dim))
    return level


def setup_inputs(seed: int = 0) -> dict:
    arg_keys = jax.random.split(jax.random.key(seed), 3)
    return {
        "positions": jnp.clip(1.0 * jax.random.uniform(arg_keys[0], (3, NX, NY, NZ, S), jnp.float32) ** block_scale(arg_keys[0], (3, NX, NY, NZ, S), ((1, 8), (2, 4), (3, 32)), -0.2, 0.2), 0.0, 1.0),
        "counts": touch_ends(jax.random.randint(arg_keys[1], (NX, NY, NZ), S * 13 // 16, S + 1), jax.random.fold_in(arg_keys[1], 1), S * 13 // 16, S).astype(jnp.int32),
    }


SENTINEL = 4.0
PAIR_SCALE = 0.02
EMBED_SCALE = 0.2
CUTOFF_SQUARED = 0.25
FORCE_SCALE = 8.0
neighbour_offsets = [(step_x, step_y, step_z) for step_x in (-1, 0, 1) for step_y in (-1, 0, 1) for step_z in (-1, 0, 1)]

def pair_geometry(own_cells, far_cells, offset):
    deltas = []
    for component in range(3):
        deltas.append(far_cells[component][..., None, :] - own_cells[component][..., :, None] + offset[component])
    return deltas

def density_terms(own_cells, far_cells, offset, itself):
    deltas = pair_geometry(own_cells, far_cells, offset)
    squared = deltas[0] * deltas[0] + deltas[1] * deltas[1] + deltas[2] * deltas[2]
    weight = jnp.maximum(1.0 - squared / CUTOFF_SQUARED, 0.0)
    square = weight * weight
    if itself:
        slot_count = own_cells.shape[-1]
        square = jnp.where(jnp.eye(slot_count, dtype=bool), 0.0, square)
    return (lax.optimization_barrier(jnp.sum(square, -1)), lax.optimization_barrier(jnp.sum(PAIR_SCALE * (square * square - 2.0 * square), -1)))

def force_terms(own_cells, far_cells, own_fp, far_fp, offset):
    deltas = pair_geometry(own_cells, far_cells, offset)
    squared = deltas[0] * deltas[0] + deltas[1] * deltas[1] + deltas[2] * deltas[2]
    weight = jnp.maximum(1.0 - squared / CUTOFF_SQUARED, 0.0)
    factor = (own_fp[..., :, None] + far_fp[..., None, :]) * (-2.0 * weight) + 4.0 * PAIR_SCALE * weight * (1.0 - weight * weight)
    return jnp.stack([FORCE_SCALE * lax.optimization_barrier(jnp.sum(factor * delta, -1)) for delta in deltas])

def neighbour(field, column, step_x, step_y, step_z):
    cells_x = field.shape[1]
    slab = lax.dynamic_index_in_dim(field, (column + step_x) % cells_x, 1, keepdims=False)
    return jnp.roll(slab, (-step_y, -step_z), axis=(1, 2))

def reference(positions, counts):
    slot_count = positions.shape[-1]
    occupied = jnp.arange(slot_count, dtype=jnp.int32) < counts[..., None]
    seated = jnp.where(occupied[None], positions, SENTINEL)
    cells_x = seated.shape[1]
    columns = jnp.arange(cells_x, dtype=jnp.int32)

    def slab_density(column):
        own_cells = lax.dynamic_index_in_dim(seated, column, 1, keepdims=False)
        rho_sum = jnp.zeros(own_cells.shape[1:], own_cells.dtype)
        pair_sum = jnp.zeros(own_cells.shape[1:], own_cells.dtype)
        for step_x, step_y, step_z in neighbour_offsets:
            far_cells = neighbour(seated, column, step_x, step_y, step_z)
            itself = step_x == 0 and step_y == 0 and (step_z == 0)
            rho_part, pair_part = density_terms(own_cells, far_cells, (step_x, step_y, step_z), itself)
            rho_sum = rho_sum + rho_part
            pair_sum = pair_sum + pair_part
        return jnp.stack([rho_sum, pair_sum])
    density = lax.map(slab_density, columns)
    rho_sum = density[:, 0]
    pair_sum = density[:, 1]
    fprime = -0.5 * EMBED_SCALE * lax.rsqrt(rho_sum + 1.0)
    energy = jnp.where(occupied, -EMBED_SCALE * jnp.sqrt(rho_sum + 1.0) + 0.5 * pair_sum, 0.0)
    fp_field = fprime[None]

    def slab_force(column):
        own_cells = lax.dynamic_index_in_dim(seated, column, 1, keepdims=False)
        own_fp = lax.dynamic_index_in_dim(fp_field, column, 1, keepdims=False)[0]
        pushes = jnp.zeros(own_cells.shape, own_cells.dtype)
        for step_x, step_y, step_z in neighbour_offsets:
            far_cells = neighbour(seated, column, step_x, step_y, step_z)
            far_fp = neighbour(fp_field, column, step_x, step_y, step_z)[0]
            pushes = pushes + force_terms(own_cells, far_cells, own_fp, far_fp, (step_x, step_y, step_z))
        return pushes
    forces = jnp.moveaxis(lax.map(slab_force, columns), 0, 1)
    forces = jnp.where(occupied[None], forces, 0.0)
    return (energy, forces)
```

```python
import jax
import jax.numpy as jnp
from jax import lax
from jax.experimental import pallas as pl
from jax.experimental.pallas import tpu as pltpu
from jax.sharding import PartitionSpec as P

SENTINEL = 4.0
S = 128
NYR = 4
NZR = 10
CELLS = NYR * NZR
SLOTS = NZR + 2
TERMS = 32
KINDS = ((0, 1), (1, 2), (2, 3), (0, 3))
PAIRS = ((1, 2), (0, 3))
USES = ((0, (0,)), (1, (0, 1)), (2, (0,)), (3, (1,)))
F32 = jnp.float32
BF16 = jnp.bfloat16


def split3(value):
    high = value.astype(BF16).astype(F32)
    rest = value - high
    mid = rest.astype(BF16).astype(F32)
    return high, mid, rest - mid


def coordinates(comps, plane):
    rows = lax.broadcasted_iota(jnp.int32, (CELLS, S), 0)
    y_row = (
        (rows >= NZR).astype(jnp.int32)
        + (rows >= 2 * NZR).astype(jnp.int32)
        + (rows >= 3 * NZR).astype(jnp.int32)
    )
    z_row = rows - NZR * y_row
    return (
        comps[0] + (plane - 0.5),
        comps[1] + (y_row.astype(F32) - 2.0),
        comps[2] + (z_row.astype(F32) - 5.0),
    )


def put_terms(t_ref, terms):
    for k, term in enumerate(terms):
        t_ref[k * CELLS : (k + 1) * CELLS, :] = term


def get_terms(t_ref, cell, count):
    return t_ref[pl.ds(cell, count, stride=CELLS), :]


def far_terms(coords):
    one = jnp.ones((CELLS, S), F32)
    zero = jnp.zeros((CELLS, S), F32)
    out = []
    for c in coords:
        h, m, l = split3(c)
        out += [h, h, h, m, m, l]
    norm = coords[0] * coords[0] + coords[1] * coords[1] + coords[2] * coords[2]
    return out + [one, one, one] + list(split3(-4.0 * norm)) + [zero] * 8


def own_terms(coords):
    one = jnp.ones((CELLS, S), F32)
    zero = jnp.zeros((CELLS, S), F32)
    out = []
    for c in coords:
        h, m, l = split3(8.0 * c)
        out += [h, m, l, h, m, h]
    norm = coords[0] * coords[0] + coords[1] * coords[1] + coords[2] * coords[2]
    return out + list(split3(1.0 - 4.0 * norm)) + [one, one, one] + [zero] * 8


def build_far(t_ref, far_ref, plane):
    def step(z, carry):
        for kind, (ya, yb) in enumerate(KINDS):
            both = jnp.concatenate(
                [get_terms(t_ref, ya * NZR + z, TERMS), get_terms(t_ref, yb * NZR + z, TERMS)], 0
            )
            at = pl.multiple_of((z + 1) * S, S)
            far_ref[plane, kind, pl.ds(at, S), :] = both.T.astype(BF16)
        return carry

    lax.fori_loop(0, NZR, step, 0)


def build_own(t_ref, own_ref):
    zero = jnp.zeros((TERMS, S), F32)

    def step(z, carry):
        for pair, (ya, yb) in enumerate(PAIRS):
            a = get_terms(t_ref, ya * NZR + z, TERMS)
            b = get_terms(t_ref, yb * NZR + z, TERMS)
            block = jnp.concatenate(
                [jnp.concatenate([a, zero], 1), jnp.concatenate([zero, b], 1)], 0
            )
            at = pl.multiple_of((z + 1) * 2 * TERMS, 2 * TERMS)
            own_ref[pair, pl.ds(at, 2 * TERMS), :] = block.astype(BF16)
        return carry

    lax.fori_loop(0, NZR, step, 0)


def fold(value):
    return jnp.sum(value.reshape(S // 8, 8, value.shape[-1]), axis=0)


def far_rows(far_ref, plane, kind, slot):
    return far_ref[plane, kind, pl.ds(pl.multiple_of(slot * S, S), S), :]


def own_block(own_ref, pair, slot):
    return own_ref[pair, pl.ds(pl.multiple_of(slot * 2 * TERMS, 2 * TERMS), 2 * TERMS), :]


def closeness(rows, block):
    return jnp.maximum(jnp.dot(rows, block, preferred_element_type=F32), 0.0)


def plane_kernel(pos_ref, far_ref, own_ref, rho_ref, quart_ref, t_ref):
    coords = coordinates([pos_ref[c] for c in range(3)], 0.0)
    for kind in range(4):
        for slot in (0, SLOTS - 1):
            far_ref[0, kind, slot * S : (slot + 1) * S, :] = jnp.zeros((S, 2 * TERMS), BF16)
    for pair in range(2):
        for slot in (0, SLOTS - 1):
            own_ref[pair, slot * 2 * TERMS : (slot + 1) * 2 * TERMS, :] = jnp.zeros(
                (2 * TERMS, 2 * S), BF16
            )
    put_terms(t_ref, far_terms(coords))
    build_far(t_ref, far_ref, 0)
    put_terms(t_ref, own_terms(coords))
    build_own(t_ref, own_ref)
    row = lax.broadcasted_iota(jnp.int32, (S, 2 * S), 0)
    lane = lax.broadcasted_iota(jnp.int32, (S, 2 * S), 1)
    itself = (row == lane) | (row + S == lane)

    def step(z, carry):
        for pair, (ya, yb) in enumerate(PAIRS):
            block = own_block(own_ref, pair, z + 1)
            rho = jnp.zeros((8, 2 * S), F32)
            quart = jnp.zeros((8, 2 * S), F32)
            for kind, pairs in USES:
                if pair not in pairs:
                    continue
                for dz in (-1, 0, 1):
                    weight = closeness(far_rows(far_ref, 0, kind, z + 1 + dz), block)
                    square = weight * weight
                    if dz == 0 and KINDS[kind] == (ya, yb):
                        square = jnp.where(itself, 0.0, square)
                    rho = rho + fold(square)
                    if pair == 0:
                        quart = quart + fold(square * square)
            rho = jnp.sum(rho, 0, keepdims=True)
            rho_ref[pl.ds(ya * NZR + z, 1), :] = rho[:, :S]
            rho_ref[pl.ds(yb * NZR + z, 1), :] = rho[:, S:]
            if pair == 0:
                quart = jnp.sum(quart, 0, keepdims=True)
                quart_ref[pl.ds(z, 1), :] = quart[:, :S]
                quart_ref[pl.ds(NZR + z, 1), :] = quart[:, S:]
        return carry

    lax.fori_loop(0, NZR, step, 0)


def column(row):
    return jnp.broadcast_to(row, (S, S)).T


def force_kernel(
    pos_ref,
    low_ref,
    high_ref,
    far0_ref,
    own_ref,
    rho_ref,
    quart_ref,
    energy_ref,
    forces_ref,
    t_ref,
    far_ref,
    xyz_ref,
    rho_sum_ref,
    quart_sum_ref,
    embed_ref,
    row_ref,
):
    sides = (low_ref, high_ref)
    for p in range(2):
        coords = coordinates([sides[p][c] for c in range(3)], (-1.0, 1.0)[p])
        put_terms(t_ref, far_terms(coords))
        build_far(t_ref, far_ref, p)

    planes = (low_ref, pos_ref, high_ref)
    for plane in range(3):
        local = [planes[plane][c] - 0.5 for c in range(3)]
        high = [v.astype(BF16).astype(F32) for v in local]
        rest = [v - h for v, h in zip(local, high)]
        put_terms(
            t_ref, high + [jnp.ones((CELLS, S), F32)] + rest + [jnp.zeros((CELLS, S), F32)]
        )

        def gather(z, carry, plane=plane):
            for kind, (ya, yb) in enumerate(KINDS[:3]):
                both = jnp.concatenate(
                    [get_terms(t_ref, ya * NZR + z, 8), get_terms(t_ref, yb * NZR + z, 8)], 0
                )
                xyz_ref[plane, kind, pl.ds(pl.multiple_of(z * 16, 16), 16), :] = both.astype(BF16)
            return carry

        lax.fori_loop(0, NZR, gather, 0)

    rho_sum_ref[...] = jnp.zeros(rho_sum_ref.shape, F32)
    quart_sum_ref[...] = jnp.zeros(quart_sum_ref.shape, F32)

    def cross(z, carry):
        for p in range(2):
            across = [jnp.zeros((S, S), F32) for _ in range(NYR)]
            for kind, pairs in USES:
                rows = far_rows(far_ref, p, kind, z + 1)
                total = None
                for dz in (-1, 0, 1):
                    for pair in pairs:
                        weight = closeness(rows, own_block(own_ref, pair, z + 1 + dz))
                        square = weight * weight
                        total = square if total is None else total + square
                        at = pl.ds(pl.multiple_of((z + 1 + dz) * 8, 8), 8)
                        rho_sum_ref[pair, at, :] += fold(square)
                        if pair == 0:
                            quart_sum_ref[at, :] += fold(square * square)
                ya, yb = KINDS[kind]
                across[ya] = across[ya] + total[:, :S]
                across[yb] = across[yb] + total[:, S:]
            for y in range(NYR):
                part = column(sides[p][3, pl.ds(y * NZR + z, 1), :])
                rho = jnp.sum(across[y], 1, keepdims=True) + part
                at = pl.multiple_of((y * NZR + z) * S, S)
                embed_ref[2 * p, pl.ds(at, S), :] = 2.5 * lax.rsqrt(rho + 1.0)
        return carry

    lax.fori_loop(0, NZR, cross, 0)

    def finish(z, carry):
        for pair, ys in enumerate(PAIRS):
            at = pl.ds(pl.multiple_of((z + 1) * 8, 8), 8)
            sums = jnp.sum(rho_sum_ref[pair, at, :], 0, keepdims=True)
            for half, y in enumerate(ys):
                rho = rho_ref[pl.ds(y * NZR + z, 1), :] + sums[:, half * S : (half + 1) * S]
                slope = 2.5 * lax.rsqrt(rho + 1.0)
                row_ref[pl.ds(y * NZR + z, 1), :] = slope
                cell_at = pl.multiple_of((y * NZR + z) * S, S)
                embed_ref[1, pl.ds(cell_at, S), :] = column(slope)
        return carry

    lax.fori_loop(0, NZR, finish, 0)

    def push(i, carry):
        z = i + 1
        rho_at = pl.ds(pl.multiple_of((z + 1) * 8, 8), 8)
        rho_both = jnp.sum(rho_sum_ref[0, rho_at, :], 0, keepdims=True)
        quart_both = jnp.sum(quart_sum_ref[rho_at, :], 0, keepdims=True)
        block = own_block(own_ref, 0, z + 1)
        own = 1.0 + jnp.concatenate(
            [row_ref[pl.ds(NZR + z, 1), :], row_ref[pl.ds(2 * NZR + z, 1), :]], 1
        )
        names = ("all", "x-", "x+", "y-", "y+", "z-", "z+")
        sums = [{n: jnp.zeros((8, S), F32) for n in names} for _ in range(2)]
        for dx in (-1, 0, 1):
            for dy in (-1, 0, 1):
                kind = dy + 1
                for dz in (-1, 0, 1):
                    if dx == 0:
                        rows = far_rows(far0_ref, 0, kind, z + 1 + dz)
                    else:
                        rows = far_rows(far_ref, (dx + 1) // 2, kind, z + 1 + dz)
                    weight = closeness(rows, block)
                    slopes = jnp.concatenate(
                        [
                            embed_ref[
                                dx + 1, pl.ds(pl.multiple_of((y * NZR + z + dz) * S, S), S), :
                            ]
                            for y in KINDS[kind]
                        ],
                        1,
                    )
                    factor = weight * ((own + slopes) - weight * weight)
                    top = factor.astype(BF16)
                    low = (factor - top.astype(F32)).astype(BF16)
                    xyz = xyz_ref[dx + 1, kind, pl.ds(pl.multiple_of((z + dz) * 16, 16), 16), :]
                    both = jnp.dot(xyz, top, preferred_element_type=F32) + jnp.dot(
                        xyz, low, preferred_element_type=F32
                    )
                    keys = ["all"]
                    keys += [axis + "-0+"[d + 1] for axis, d in zip("xyz", (dx, dy, dz)) if d]
                    for half in range(2):
                        part = both[half * 8 : half * 8 + 8, half * S : half * S + S]
                        for key in keys:
                            sums[half][key] = sums[half][key] + part
        for half in range(2):
            y = half + 1
            at = pl.ds(y * NZR + z, 1)
            occupied = pos_ref[0, at, :] < 2.0
            acc = sums[half]
            weight_sum = acc["all"][3:4]
            for c, axis in enumerate("xyz"):
                moved = acc[axis + "+"][3:4] - acc[axis + "-"][3:4]
                centre = acc["all"][c : c + 1] + acc["all"][c + 4 : c + 5]
                force = (centre + moved) - (pos_ref[c, at, :] - 0.5) * weight_sum
                forces_ref[pl.ds((c * 2 + half) * 8 + i, 1), :] = jnp.where(
                    occupied, 0.64 * force, 0.0
                )
            rho = rho_ref[at, :] + rho_both[:, half * S : (half + 1) * S]
            quart = quart_ref[pl.ds(half * NZR + z, 1), :] + quart_both[:, half * S : (half + 1) * S]
            energy = -0.2 * jnp.sqrt(rho + 1.0) + 0.01 * (quart - 2.0 * rho)
            energy_ref[pl.ds(half * 8 + i, 1), :] = jnp.where(occupied, energy, 0.0)
        return carry

    lax.fori_loop(0, NZR - 2, push, 0)


def ring(axis, step):
    count = lax.axis_size(axis)
    return [(i, (i + step) % count) for i in range(count)]


def widen(block, axis, dim):
    low = lax.ppermute(
        lax.slice_in_dim(block, block.shape[dim] - 1, None, axis=dim), axis, ring(axis, 1)
    )
    high = lax.ppermute(lax.slice_in_dim(block, 0, 1, axis=dim), axis, ring(axis, -1))
    return jnp.concatenate([low, block, high], axis=dim)


def plane_sums(plane):
    return pl.pallas_call(
        plane_kernel,
        out_shape=(
            jax.ShapeDtypeStruct((1, 4, SLOTS * S, 2 * TERMS), BF16),
            jax.ShapeDtypeStruct((2, SLOTS * 2 * TERMS, 2 * S), BF16),
            jax.ShapeDtypeStruct((CELLS, S), F32),
            jax.ShapeDtypeStruct((2 * NZR, S), F32),
        ),
        scratch_shapes=[pltpu.VMEM((TERMS * CELLS, S), F32)],
        name="plane",
    )(plane)


def finish_forces(*operands):
    return pl.pallas_call(
        force_kernel,
        out_shape=(
            jax.ShapeDtypeStruct((2 * 8, S), F32),
            jax.ShapeDtypeStruct((3 * 2 * 8, S), F32),
        ),
        scratch_shapes=[
            pltpu.VMEM((TERMS * CELLS, S), F32),
            pltpu.VMEM((2, 4, SLOTS * S, 2 * TERMS), BF16),
            pltpu.VMEM((3, 3, NZR * 16, S), BF16),
            pltpu.VMEM((2, SLOTS * 8, 2 * S), F32),
            pltpu.VMEM((SLOTS * 8, 2 * S), F32),
            pltpu.VMEM((3, CELLS * S, S), F32),
            pltpu.VMEM((CELLS, S), F32),
        ],
        name="forces",
    )(*operands)


def per_device(positions, counts):
    occupied = jnp.arange(S, dtype=jnp.int32) < counts[..., None]
    seated = jnp.where(occupied[None], positions, SENTINEL)[:, 0]
    plane = widen(widen(seated, "gz", 2), "gy", 1).reshape(3, CELLS, S)
    far0, own, rho, quart = plane_sums(plane)
    message = jnp.concatenate([plane, rho[None]], 0)
    low = lax.ppermute(message, "gx", ring("gx", 1))
    high = lax.ppermute(message, "gx", ring("gx", -1))
    energy, forces = finish_forces(plane, low, high, far0, own, rho, quart)
    return (energy.reshape(1, 2, 8, S), forces.reshape(3, 1, 2, 8, S))


def solution(mesh):
    placed = (P(None, "gx", "gy", "gz", None), P("gx", "gy", "gz"))
    return jax.shard_map(
        per_device,
        mesh=mesh,
        in_specs=placed,
        out_specs=(P("gx", "gy", "gz", None), P(None, "gx", "gy", "gz", None)),
        check_vma=False,
    )
```

```python
import functools

import jax
import jax.numpy as jnp
from jax import lax
from jax.experimental import pallas as pl
from jax.experimental.pallas import tpu as pltpu
from jax.sharding import PartitionSpec as P

SENTINEL = 4.0
S = 128
NYR = 4
NZR = 10
CELLS = NYR * NZR
SLOTS = NZR + 2
TERMS = 32
KINDS = ((0, 1), (1, 2), (2, 3), (0, 3))
PAIRS = ((1, 2), (0, 3))
USES = ((0, (0,)), (1, (0, 1)), (2, (0,)), (3, (1,)))
TIERS = (80, 96, S)
OWN = 16
ROLL = 80
VMEM_LIMIT = 24 * 2**20
F32 = jnp.float32
BF16 = jnp.bfloat16


def split3(value):
    high = value.astype(BF16).astype(F32)
    rest = value - high
    mid = rest.astype(BF16).astype(F32)
    return high, mid, rest - mid


def coordinates(comps, plane):
    rows = lax.broadcasted_iota(jnp.int32, (CELLS, S), 0)
    y_row = (
        (rows >= NZR).astype(jnp.int32)
        + (rows >= 2 * NZR).astype(jnp.int32)
        + (rows >= 3 * NZR).astype(jnp.int32)
    )
    z_row = rows - NZR * y_row
    return (
        comps[0] + (plane - 0.5),
        comps[1] + (y_row.astype(F32) - 2.0),
        comps[2] + (z_row.astype(F32) - 5.0),
    )


def put_terms(t_ref, terms):
    for k, term in enumerate(terms):
        t_ref[k * CELLS : (k + 1) * CELLS, :] = term


def get_terms(t_ref, cell, count):
    return t_ref[pl.ds(cell, count, stride=CELLS), :]


def far_terms(coords):
    one = jnp.ones((CELLS, S), F32)
    zero = jnp.zeros((CELLS, S), F32)
    out = []
    for c in coords:
        h, m, l = split3(c)
        out += [h, h, h, m, m, l]
    norm = coords[0] * coords[0] + coords[1] * coords[1] + coords[2] * coords[2]
    return out + [one, one, one] + list(split3(-4.0 * norm)) + [zero] * 8


def own_terms(coords):
    one = jnp.ones((CELLS, S), F32)
    zero = jnp.zeros((CELLS, S), F32)
    out = []
    for c in coords:
        h, m, l = split3(8.0 * c)
        out += [h, m, l, h, m, h]
    norm = coords[0] * coords[0] + coords[1] * coords[1] + coords[2] * coords[2]
    return out + list(split3(1.0 - 4.0 * norm)) + [one, one, one] + [zero] * 8


def build_far(t_ref, far_refs, kinds, rows=S):
    def step(z, carry):
        for kind, far_ref in zip(kinds, far_refs):
            ya, yb = KINDS[kind]
            both = jnp.concatenate(
                [get_terms(t_ref, ya * NZR + z, TERMS), get_terms(t_ref, yb * NZR + z, TERMS)], 0
            )
            at = pl.multiple_of((z + 1) * S, S)
            far_ref[pl.ds(at, rows), :] = both.T[:rows].astype(BF16)
        return carry

    lax.fori_loop(0, NZR, step, 0)


def build_own(t_ref, own_ref, pair):
    zero = jnp.zeros((TERMS, S), F32)
    ya, yb = PAIRS[pair]

    def step(z, carry):
        a = get_terms(t_ref, ya * NZR + z, TERMS)
        b = get_terms(t_ref, yb * NZR + z, TERMS)
        block = jnp.concatenate([jnp.concatenate([a, zero], 1), jnp.concatenate([zero, b], 1)], 0)
        at = pl.multiple_of((z + 1) * 2 * TERMS, 2 * TERMS)
        own_ref[pl.ds(at, 2 * TERMS), :] = block.astype(BF16)
        return carry

    lax.fori_loop(0, NZR, step, 0)


def empty_ends(ref, size):
    for slot in (0, SLOTS - 1):
        ref[slot * size : (slot + 1) * size, :] = jnp.zeros((size, ref.shape[1]), BF16)


def fold(value):
    return jnp.sum(value.reshape(value.shape[0] // 8, 8, value.shape[-1]), axis=0)


def far_rows(far_ref, slot, rows=S):
    return far_ref[pl.ds(pl.multiple_of(slot * S, S), rows), :]


def own_block(own_ref, slot):
    return own_ref[pl.ds(pl.multiple_of(slot * 2 * TERMS, 2 * TERMS), 2 * TERMS), :]


def closeness(rows, block):
    return jnp.maximum(jnp.dot(rows, block, preferred_element_type=F32), 0.0)


def sort_kernel(pos_ref, counts_ref, own_ref, rank_ref, t_ref):
    lane = lax.broadcasted_iota(jnp.int32, (OWN, S), 1)
    occupied = lane < counts_ref[...]
    comps = [jnp.where(occupied, pos_ref[c], SENTINEL) for c in range(3)]
    low = occupied & (comps[0] < 0.5)
    high = occupied & (comps[0] >= 0.5)
    up_to = lax.broadcasted_iota(jnp.int32, (S, S), 0) <= lax.broadcasted_iota(
        jnp.int32, (S, S), 1
    )
    up_to = jnp.where(up_to, 1.0, 0.0).astype(BF16)
    flags = jnp.concatenate([jnp.where(m, 1.0, 0.0) for m in (low, high, ~occupied)], 0)
    before = jnp.dot(flags.astype(BF16), up_to, preferred_element_type=F32)
    lows, highs, blanks = before[:OWN], before[OWN : 2 * OWN], before[2 * OWN :]
    all_low = jnp.max(lows, axis=1, keepdims=True)
    rank = jnp.where(low, lows - 1.0, jnp.where(high, S - highs, all_low + blanks - 1.0))
    rank_ref[...] = rank
    terms = []
    for c in comps:
        terms += list(split3(c))
    for k, term in enumerate(terms + [jnp.zeros((OWN, S), F32)] * 7):
        t_ref[k * OWN : (k + 1) * OWN, :] = term
    slot = lax.broadcasted_iota(jnp.int32, (S, S), 0).astype(F32)
    for cell in range(OWN):
        chosen = jnp.where(slot == rank[cell : cell + 1], 1.0, 0.0).astype(BF16)
        rows = t_ref[pl.ds(cell, 16, stride=OWN), :].astype(BF16)
        moved = lax.dot_general(
            rows, chosen, (((1,), (1,)), ((), ())), preferred_element_type=F32
        )
        for c in range(3):
            own_ref[c, cell : cell + 1, :] = (
                moved[3 * c : 3 * c + 1] + moved[3 * c + 1 : 3 * c + 2]
            ) + moved[3 * c + 2 : 3 * c + 3]


def row_sums(z, far_refs, kinds, own_ref, pair, rho, quart):
    block = own_block(own_ref, z + 1)
    row = lax.broadcasted_iota(jnp.int32, (S, 2 * S), 0)
    lane = lax.broadcasted_iota(jnp.int32, (S, 2 * S), 1)
    itself = (row == lane) | (row + S == lane)
    for kind, far_ref in zip(kinds, far_refs):
        for dz in (-1, 0, 1):
            weight = closeness(far_rows(far_ref, z + 1 + dz), block)
            square = weight * weight
            if dz == 0 and KINDS[kind] == PAIRS[pair]:
                square = jnp.where(itself, 0.0, square)
            rho = rho + fold(square)
            if pair == 0:
                quart = quart + fold(square * square)
    return jnp.sum(rho, 0, keepdims=True), jnp.sum(quart, 0, keepdims=True)


def pair_row_kernel(pos_ref, far_ref, own_ref, sums_ref, t_ref, whole_ref):
    for c in range(3):
        for y in range(2):
            whole_ref[c, (y + 1) * NZR : (y + 2) * NZR, :] = pos_ref[c, y]
            whole_ref[c, y * 3 * NZR : (y * 3 + 1) * NZR, :] = jnp.zeros((NZR, S), F32)
    coords = coordinates([whole_ref[c] for c in range(3)], 0.0)
    empty_ends(far_ref, S)
    empty_ends(own_ref, 2 * TERMS)
    put_terms(t_ref, far_terms(coords))
    build_far(t_ref, [far_ref], [1])
    put_terms(t_ref, own_terms(coords))
    build_own(t_ref, own_ref, 0)
    zero = jnp.zeros((8, 2 * S), F32)

    def step(z, carry):
        rho, quart = row_sums(z, [far_ref], [1], own_ref, 0, zero, zero)
        sums_ref[pl.ds(z, 1), :] = rho
        sums_ref[pl.ds(NZR + z, 1), :] = quart
        return carry

    lax.fori_loop(0, NZR, step, 0)


def plane_kernel(
    pos_ref,
    below_ref,
    above_ref,
    mid_ref,
    own_ref,
    sums_ref,
    plane_ref,
    far_a_ref,
    far_b_ref,
    own_halo_ref,
    quart_ref,
    t_ref,
    far_c_ref,
):
    for c in range(3):
        plane_ref[c, 0:NZR, :] = below_ref[c, 0]
        plane_ref[c, NZR : 2 * NZR, :] = pos_ref[c, 0]
        plane_ref[c, 2 * NZR : 3 * NZR, :] = pos_ref[c, 1]
        plane_ref[c, 3 * NZR :, :] = above_ref[c, 0]
    coords = coordinates([plane_ref[c] for c in range(3)], 0.0)
    for ref in (far_a_ref, far_b_ref, far_c_ref):
        empty_ends(ref, S)
    empty_ends(own_halo_ref, 2 * TERMS)
    put_terms(t_ref, far_terms(coords))
    build_far(t_ref, [far_a_ref, far_b_ref, far_c_ref], [0, 2, 3])
    put_terms(t_ref, own_terms(coords))
    build_own(t_ref, own_halo_ref, 1)
    zero = jnp.zeros((8, 2 * S), F32)

    def step(z, carry):
        rho, quart = row_sums(z, [far_a_ref, far_b_ref], [0, 2], own_ref, 0, zero, zero)
        rho = rho + sums_ref[pl.ds(z, 1), :]
        quart = quart + sums_ref[pl.ds(NZR + z, 1), :]
        plane_ref[3, pl.ds(NZR + z, 1), :] = rho[:, :S]
        plane_ref[3, pl.ds(2 * NZR + z, 1), :] = rho[:, S:]
        quart_ref[pl.ds(z, 1), :] = quart[:, :S]
        quart_ref[pl.ds(NZR + z, 1), :] = quart[:, S:]
        rho, _ = row_sums(z, [mid_ref, far_c_ref], [1, 3], own_halo_ref, 1, zero, zero)
        plane_ref[3, pl.ds(z, 1), :] = rho[:, :S]
        plane_ref[3, pl.ds(3 * NZR + z, 1), :] = rho[:, S:]
        return carry

    lax.fori_loop(0, NZR, step, 0)


def column(row, rows=S):
    return jnp.broadcast_to(row, (S, S)).T[:rows]


def force_kernel(
    plane_ref,
    low_ref,
    high_ref,
    mid_ref,
    far_a_ref,
    far_b_ref,
    own_ref,
    own_halo_ref,
    quart_ref,
    rank_ref,
    energy_ref,
    forces_ref,
    t_ref,
    rolled_ref,
    far_ref,
    xyz_ref,
    rho_sum_ref,
    quart_sum_ref,
    embed_ref,
    row_ref,
    done_ref,
):
    lane = lax.broadcasted_iota(jnp.int32, (CELLS, S), 1)
    for c in range(4):
        rolled_ref[c] = pltpu.roll(low_ref[c], ROLL, 1)
    x_low, x_high = rolled_ref[0], high_ref[0]
    last = jnp.maximum(
        jnp.where((x_low > 0.5) & (x_low < 2.0), lane, -1),
        jnp.where(x_high < 0.5, lane, -1),
    )
    needed = jnp.max(last) + 1
    own_pairs = (own_ref, own_halo_ref)
    far0 = (far_a_ref, mid_ref, far_b_ref)
    sides = (rolled_ref, high_ref)
    rho_sum_ref[...] = jnp.zeros(rho_sum_ref.shape, F32)
    quart_sum_ref[...] = jnp.zeros(quart_sum_ref.shape, F32)

    planes = (rolled_ref, plane_ref, high_ref)
    for plane in range(3):
        local = [planes[plane][c] - 0.5 for c in range(3)]
        high = [v.astype(BF16).astype(F32) for v in local]
        rest = [v - h for v, h in zip(local, high)]
        put_terms(
            t_ref, high + [jnp.ones((CELLS, S), F32)] + rest + [jnp.zeros((CELLS, S), F32)]
        )

        def gather(z, carry, plane=plane):
            for kind, (ya, yb) in enumerate(KINDS[:3]):
                both = jnp.concatenate(
                    [get_terms(t_ref, ya * NZR + z, 8), get_terms(t_ref, yb * NZR + z, 8)], 0
                )
                xyz_ref[plane, kind, pl.ds(pl.multiple_of(z * 16, 16), 16), :] = both.astype(BF16)
            return carry

        lax.fori_loop(0, NZR, gather, 0)

    def with_rows(count):
        for p in range(2):
            coords = coordinates([sides[p][c] for c in range(3)], (-1.0, 1.0)[p])
            put_terms(t_ref, far_terms(coords))
            build_far(t_ref, [far_ref.at[p, k] for k in range(4)], range(4), count)

        def cross(z, carry):
            for p in range(2):
                across = [None] * NYR
                for kind, pairs in USES:
                    rows = far_rows(far_ref.at[p, kind], z + 1, count)
                    total = None
                    for dz in (-1, 0, 1):
                        for pair in pairs:
                            weight = closeness(rows, own_block(own_pairs[pair], z + 1 + dz))
                            square = weight * weight
                            total = square if total is None else total + square
                            at = pl.ds(pl.multiple_of((z + 1 + dz) * 8, 8), 8)
                            rho_sum_ref[pair, at, :] += fold(square)
                            if pair == 0:
                                quart_sum_ref[at, :] += fold(square * square)
                    for half, y in enumerate(KINDS[kind]):
                        part = total[:, half * S : (half + 1) * S]
                        across[y] = part if across[y] is None else across[y] + part
                for y in range(NYR):
                    part = column(sides[p][3, pl.ds(y * NZR + z, 1), :], count)
                    rho = jnp.sum(across[y], 1, keepdims=True) + part
                    at = pl.multiple_of((y * NZR + z) * S, S)
                    embed_ref[2 * p, pl.ds(at, count), :] = 2.5 * lax.rsqrt(rho + 1.0)
            return carry

        lax.fori_loop(0, NZR, cross, 0)

        def finish(z, carry):
            for pair, ys in enumerate(PAIRS):
                at = pl.ds(pl.multiple_of((z + 1) * 8, 8), 8)
                sums = jnp.sum(rho_sum_ref[pair, at, :], 0, keepdims=True)
                for half, y in enumerate(ys):
                    rho = plane_ref[3, pl.ds(y * NZR + z, 1), :] + sums[:, half * S : half * S + S]
                    slope = 2.5 * lax.rsqrt(rho + 1.0)
                    row_ref[pl.ds(y * NZR + z, 1), :] = slope
                    cell_at = pl.multiple_of((y * NZR + z) * S, S)
                    embed_ref[1, pl.ds(cell_at, S), :] = column(slope)
            return carry

        lax.fori_loop(0, NZR, finish, 0)

        def push(i, carry):
            z = i + 1
            rho_at = pl.ds(pl.multiple_of((z + 1) * 8, 8), 8)
            rho_both = jnp.sum(rho_sum_ref[0, rho_at, :], 0, keepdims=True)
            quart_both = jnp.sum(quart_sum_ref[rho_at, :], 0, keepdims=True)
            block = own_block(own_ref, z + 1)
            own = 1.0 + jnp.concatenate(
                [row_ref[pl.ds(NZR + z, 1), :], row_ref[pl.ds(2 * NZR + z, 1), :]], 1
            )
            names = ("all", "x-", "x+", "y-", "y+", "z-", "z+")
            sums = [{n: jnp.zeros((8, S), F32) for n in names} for _ in range(2)]
            for dx in (-1, 0, 1):
                used = S if dx == 0 else count
                for dy in (-1, 0, 1):
                    kind = dy + 1
                    for dz in (-1, 0, 1):
                        if dx == 0:
                            rows = far_rows(far0[kind], z + 1 + dz)
                        else:
                            rows = far_rows(far_ref.at[(dx + 1) // 2, kind], z + 1 + dz, count)
                        weight = closeness(rows, block)
                        slopes = jnp.concatenate(
                            [
                                embed_ref[
                                    dx + 1,
                                    pl.ds(pl.multiple_of((y * NZR + z + dz) * S, S), used),
                                    :,
                                ]
                                for y in KINDS[kind]
                            ],
                            1,
                        )
                        factor = weight * ((own + slopes) - weight * weight)
                        top = factor.astype(BF16)
                        low = (factor - top.astype(F32)).astype(BF16)
                        xyz = xyz_ref[
                            dx + 1, kind, pl.ds(pl.multiple_of((z + dz) * 16, 16), 16), :
                        ][:, :used]
                        both = jnp.dot(xyz, top, preferred_element_type=F32) + jnp.dot(
                            xyz, low, preferred_element_type=F32
                        )
                        keys = ["all"]
                        keys += [a + "-0+"[d + 1] for a, d in zip("xyz", (dx, dy, dz)) if d]
                        for half in range(2):
                            part = both[half * 8 : half * 8 + 8, half * S : half * S + S]
                            for key in keys:
                                sums[half][key] = sums[half][key] + part
            for half in range(2):
                y = half + 1
                at = pl.ds(y * NZR + z, 1)
                occupied = plane_ref[0, at, :] < 2.0
                acc = sums[half]
                weight_sum = acc["all"][3:4]
                rho = plane_ref[3, at, :] + rho_both[:, half * S : (half + 1) * S]
                quart = (
                    quart_ref[pl.ds(half * NZR + z, 1), :]
                    + quart_both[:, half * S : (half + 1) * S]
                )
                results = [-0.2 * jnp.sqrt(rho + 1.0) + 0.01 * (quart - 2.0 * rho)]
                for c, axis in enumerate("xyz"):
                    moved = acc[axis + "+"][3:4] - acc[axis + "-"][3:4]
                    centre = acc["all"][c : c + 1] + acc["all"][c + 4 : c + 5]
                    force = (centre + moved) - (plane_ref[c, at, :] - 0.5) * weight_sum
                    results.append(0.64 * force)
                for k, result in enumerate(results):
                    done_ref[pl.ds(k * OWN + half * 8 + i, 1), :] = jnp.where(
                        occupied, result, 0.0
                    )
            return carry

        lax.fori_loop(0, NZR - 2, push, 0)

    floor = 0
    for count in TIERS:
        pl.when((needed > floor if floor else needed >= 0) & (needed <= count))(
            functools.partial(with_rows, count)
        )
        floor = count

    for k, part in enumerate(split3(done_ref[...])):
        t_ref[k * 4 * OWN : (k + 1) * 4 * OWN, :] = part
    slot = lax.broadcasted_iota(jnp.int32, (S, S), 0).astype(F32)
    for cell in range(OWN):
        chosen = jnp.where(slot == rank_ref[cell : cell + 1, :], 1.0, 0.0).astype(BF16)
        rows = t_ref[pl.ds(cell, 16, stride=OWN), :].astype(BF16)
        moved = jnp.dot(rows, chosen, preferred_element_type=F32)
        moved = (moved[0:4] + moved[4:8]) + moved[8:12]
        energy_ref[cell : cell + 1, :] = moved[0:1]
        for c in range(3):
            forces_ref[c * OWN + cell : c * OWN + cell + 1, :] = moved[c + 1 : c + 2]


def ring(axis, step):
    count = lax.axis_size(axis)
    return [(i, (i + step) % count) for i in range(count)]


def kernel_call(body, outs, scratch, name):
    return pl.pallas_call(
        body,
        out_shape=tuple(jax.ShapeDtypeStruct(shape, dtype) for shape, dtype in outs),
        scratch_shapes=[pltpu.VMEM(shape, dtype) for shape, dtype in scratch],
        compiler_params=pltpu.CompilerParams(vmem_limit_bytes=VMEM_LIMIT),
        name=name,
    )


FAR = ((SLOTS * S, 2 * TERMS), BF16)
OWN_BLOCKS = ((SLOTS * 2 * TERMS, 2 * S), BF16)
TERM_ROWS = ((TERMS * CELLS, S), F32)


def sort_cells(positions, counts):
    return kernel_call(
        sort_kernel, [((3, OWN, S), F32), ((OWN, S), F32)], [((16 * OWN, S), F32)], "sort"
    )(positions, counts)


def pair_row(rows):
    return kernel_call(
        pair_row_kernel,
        [FAR, OWN_BLOCKS, ((2 * NZR, 2 * S), F32)],
        [TERM_ROWS, ((3, CELLS, S), F32)],
        "rows",
    )(rows)


def plane_sums(rows, below, above, mid, own, sums):
    return kernel_call(
        plane_kernel,
        [((4, CELLS, S), F32), FAR, FAR, OWN_BLOCKS, ((2 * NZR, S), F32)],
        [TERM_ROWS, FAR],
        "plane",
    )(rows, below, above, mid, own, sums)


def finish_forces(*operands):
    return kernel_call(
        force_kernel,
        [((OWN, S), F32), ((3 * OWN, S), F32)],
        [
            TERM_ROWS,
            ((4, CELLS, S), F32),
            ((2, 4, SLOTS * S, 2 * TERMS), BF16),
            ((3, 3, NZR * 16, S), BF16),
            ((2, SLOTS * 8, 2 * S), F32),
            ((SLOTS * 8, 2 * S), F32),
            ((3, CELLS * S, S), F32),
            ((CELLS, S), F32),
            ((4 * OWN, S), F32),
        ],
        "forces",
    )(*operands)


def per_device(positions, counts):
    sorted_own, rank = sort_cells(positions.reshape(3, OWN, S), counts.reshape(OWN, 1))
    cells = sorted_own.reshape(3, 2, 8, S)
    behind = lax.ppermute(cells[:, :, 7:8], "gz", ring("gz", 1))
    ahead = lax.ppermute(cells[:, :, 0:1], "gz", ring("gz", -1))
    rows = jnp.concatenate([behind, cells, ahead], axis=2)
    below = lax.ppermute(rows[:, 1:2], "gy", ring("gy", 1))
    above = lax.ppermute(rows[:, 0:1], "gy", ring("gy", -1))
    mid, own, sums = pair_row(rows)
    plane, far_a, far_b, own_halo, quart = plane_sums(rows, below, above, mid, own, sums)
    low = lax.ppermute(plane, "gx", ring("gx", 1))
    high = lax.ppermute(plane, "gx", ring("gx", -1))
    energy, forces = finish_forces(
        plane, low, high, mid, far_a, far_b, own, own_halo, quart, rank
    )
    return (energy.reshape(1, 2, 8, S), forces.reshape(3, 1, 2, 8, S))


def solution(mesh):
    placed = (P(None, "gx", "gy", "gz", None), P("gx", "gy", "gz"))
    return jax.shard_map(
        per_device,
        mesh=mesh,
        in_specs=placed,
        out_specs=(P("gx", "gy", "gz", None), P(None, "gx", "gy", "gz", None)),
        check_vma=False,
    )
```

```python
import functools

import jax
import jax.numpy as jnp
from jax import lax
from jax.experimental import pallas as pl
from jax.experimental.pallas import tpu as pltpu
from jax.sharding import PartitionSpec as P

SENTINEL = 4.0
S = 128
NYR = 4
NZR = 10
CELLS = NYR * NZR
SLOTS = NZR + 2
TERMS = 32
KINDS = ((0, 1), (1, 2), (2, 3), (0, 3))
PAIRS = ((1, 2), (0, 3))
USES = ((0, (0,)), (1, (0, 1)), (2, (0,)), (3, (1,)))
TIERS = (80, 96, S)
OWN = 16
VMEM_LIMIT = 24 * 2**20
F32 = jnp.float32
BF16 = jnp.bfloat16


def split3(value):
    high = value.astype(BF16).astype(F32)
    rest = value - high
    mid = rest.astype(BF16).astype(F32)
    return high, mid, rest - mid


def coordinates(comps, plane):
    rows = lax.broadcasted_iota(jnp.int32, (CELLS, S), 0)
    y_row = (
        (rows >= NZR).astype(jnp.int32)
        + (rows >= 2 * NZR).astype(jnp.int32)
        + (rows >= 3 * NZR).astype(jnp.int32)
    )
    z_row = rows - NZR * y_row
    return (
        comps[0] + (plane - 0.5),
        comps[1] + (y_row.astype(F32) - 2.0),
        comps[2] + (z_row.astype(F32) - 5.0),
    )


def put_terms(t_ref, terms):
    for k, term in enumerate(terms):
        t_ref[k * CELLS : (k + 1) * CELLS, :] = term


def get_terms(t_ref, cell, count):
    return t_ref[pl.ds(cell, count, stride=CELLS), :]


def far_terms(coords):
    one = jnp.ones((CELLS, S), F32)
    zero = jnp.zeros((CELLS, S), F32)
    out = []
    for c in coords:
        h, m, l = split3(c)
        out += [h, h, h, m, m, l]
    norm = coords[0] * coords[0] + coords[1] * coords[1] + coords[2] * coords[2]
    return out + [one, one, one] + list(split3(-4.0 * norm)) + [zero] * 8


def own_terms(coords):
    one = jnp.ones((CELLS, S), F32)
    zero = jnp.zeros((CELLS, S), F32)
    out = []
    for c in coords:
        h, m, l = split3(8.0 * c)
        out += [h, m, l, h, m, h]
    norm = coords[0] * coords[0] + coords[1] * coords[1] + coords[2] * coords[2]
    return out + list(split3(1.0 - 4.0 * norm)) + [one, one, one] + [zero] * 8


def build_far(t_ref, far_refs, rows=S):
    low_half = lax.broadcasted_iota(jnp.int32, (rows, 2 * TERMS), 1) < TERMS

    def step(z, carry):
        sides = []
        for y in (0, 2):
            both = jnp.concatenate(
                [get_terms(t_ref, y * NZR + z, TERMS), get_terms(t_ref, (y + 1) * NZR + z, TERMS)],
                0,
            )
            sides.append(both.T[:rows])
        at = pl.multiple_of((z + 1) * S, S)
        for far_ref, first, second in zip(far_refs, (0, 1, 1, 0), (0, 0, 1, 1)):
            if far_ref is None:
                continue
            value = sides[first]
            if first != second:
                value = jnp.where(low_half, sides[first], sides[second])
            far_ref[pl.ds(at, rows), :] = value.astype(BF16)
        return carry

    lax.fori_loop(0, NZR, step, 0, unroll=5)


def build_own(t_ref, own_ref, pair):
    zero = jnp.zeros((TERMS, S), F32)
    ya, yb = PAIRS[pair]

    def step(z, carry):
        a = get_terms(t_ref, ya * NZR + z, TERMS)
        b = get_terms(t_ref, yb * NZR + z, TERMS)
        a = jnp.concatenate([a, zero], 1).astype(BF16)
        b = jnp.concatenate([zero, b], 1).astype(BF16)
        at = pl.multiple_of((z + 1) * 2 * TERMS, 2 * TERMS)
        own_ref[0, pl.ds(at, 2 * TERMS), :] = jnp.concatenate([a, b], 0)
        own_ref[1, pl.ds(at, 2 * TERMS), :] = jnp.concatenate([b, a], 0)
        return carry

    lax.fori_loop(0, NZR, step, 0, unroll=5)


def empty_ends(ref, size):
    for slot in (0, SLOTS - 1):
        ref[slot * size : (slot + 1) * size, :] = jnp.zeros((size, ref.shape[1]), BF16)


def fold(value):
    return jnp.sum(value.reshape(value.shape[0] // 8, 8, value.shape[-1]), axis=0)


def far_rows(far_ref, slot, rows=S):
    return far_ref[pl.ds(pl.multiple_of(slot * S, S), rows), :]


def own_block(own_ref, slot, kind):
    at = pl.multiple_of(slot * 2 * TERMS, 2 * TERMS)
    return own_ref[1 if kind == 1 else 0, pl.ds(at, 2 * TERMS), :]


def closeness(rows, block):
    return jnp.maximum(jnp.dot(rows, block, preferred_element_type=F32), 0.0)


def sort_kernel(pos_hbm, counts_hbm, own_ref, rank_ref, t_ref, pos_ref, counts_ref, sem_p, sem_c):
    copy_p = pltpu.make_async_copy(pos_hbm, pos_ref, sem_p)
    copy_c = pltpu.make_async_copy(counts_hbm, counts_ref, sem_c)
    copy_p.start()
    copy_c.start()
    copy_p.wait()
    copy_c.wait()
    lane = lax.broadcasted_iota(jnp.int32, (OWN, S), 1)
    row = lax.broadcasted_iota(jnp.int32, (OWN, S), 0)
    held = jnp.zeros((OWN, S), jnp.int32)
    for cell in range(OWN):
        held = jnp.where(row == cell, counts_ref[0, cell // 8, cell % 8], held)
    occupied = lane < held
    comps = [
        jnp.where(occupied, jnp.concatenate([pos_ref[c, 0, 0], pos_ref[c, 0, 1]], 0), SENTINEL)
        for c in range(3)
    ]
    low = occupied & (comps[0] < 0.5)
    high = occupied & (comps[0] >= 0.5)
    up_to = lax.broadcasted_iota(jnp.int32, (S, S), 0) <= lax.broadcasted_iota(
        jnp.int32, (S, S), 1
    )
    up_to = jnp.where(up_to, 1.0, 0.0).astype(BF16)
    flags = jnp.concatenate([jnp.where(m, 1.0, 0.0) for m in (low, high, ~occupied)], 0)
    before = jnp.dot(flags.astype(BF16), up_to, preferred_element_type=F32)
    lows, highs, blanks = before[:OWN], before[OWN : 2 * OWN], before[2 * OWN :]
    all_low = jnp.max(lows, axis=1, keepdims=True)
    rank = jnp.where(low, lows - 1.0, jnp.where(high, S - highs, all_low + blanks - 1.0))
    rank_ref[...] = rank
    terms = []
    for c in comps:
        terms += list(split3(c))
    for k, term in enumerate(terms + [jnp.zeros((OWN, S), F32)] * 7):
        t_ref[k * OWN : (k + 1) * OWN, :] = term
    slot = lax.broadcasted_iota(jnp.int32, (S, S), 0).astype(F32)
    for cell in range(OWN):
        chosen = jnp.where(slot == rank[cell : cell + 1], 1.0, 0.0).astype(BF16)
        rows = t_ref[pl.ds(cell, 16, stride=OWN), :].astype(BF16)
        moved = lax.dot_general(
            rows, chosen, (((1,), (1,)), ((), ())), preferred_element_type=F32
        )
        for c in range(3):
            own_ref[c, cell : cell + 1, :] = (
                moved[3 * c : 3 * c + 1] + moved[3 * c + 1 : 3 * c + 2]
            ) + moved[3 * c + 2 : 3 * c + 3]


def row_sums(z, far_refs, kinds, own_ref, pair, rho, quart):
    row = lax.broadcasted_iota(jnp.int32, (S, 2 * S), 0)
    lane = lax.broadcasted_iota(jnp.int32, (S, 2 * S), 1)
    itself = (row == lane) | (row + S == lane)
    for kind, far_ref in zip(kinds, far_refs):
        for dz in (-1, 0, 1):
            weight = closeness(far_rows(far_ref, z + 1 + dz), own_block(own_ref, z + 1, kind))
            square = weight * weight
            if dz == 0 and KINDS[kind] == PAIRS[pair]:
                square = jnp.where(itself, 0.0, square)
            rho = rho + fold(square)
            if pair == 0:
                quart = quart + fold(square * square)
    return jnp.sum(rho, 0, keepdims=True), jnp.sum(quart, 0, keepdims=True)


def pair_row_kernel(pos_ref, far_ref, own_ref, sums_ref, t_ref, whole_ref):
    for c in range(3):
        for y in range(2):
            whole_ref[c, (y + 1) * NZR : (y + 2) * NZR, :] = pos_ref[c, y]
            whole_ref[c, y * 3 * NZR : (y * 3 + 1) * NZR, :] = jnp.zeros((NZR, S), F32)
    coords = coordinates([whole_ref[c] for c in range(3)], 0.0)
    empty_ends(far_ref, S)
    empty_ends(own_ref.at[0], 2 * TERMS)
    empty_ends(own_ref.at[1], 2 * TERMS)
    put_terms(t_ref, far_terms(coords))
    build_far(t_ref, [None, far_ref, None, None])
    put_terms(t_ref, own_terms(coords))
    build_own(t_ref, own_ref, 0)
    zero = jnp.zeros((8, 2 * S), F32)

    def step(z, carry):
        rho, quart = row_sums(z, [far_ref], [1], own_ref, 0, zero, zero)
        sums_ref[pl.ds(z, 1), :] = rho
        sums_ref[pl.ds(NZR + z, 1), :] = quart
        return carry

    lax.fori_loop(0, NZR, step, 0, unroll=5)


def plane_kernel(
    pos_ref,
    below_ref,
    above_ref,
    mid_ref,
    own_ref,
    sums_ref,
    plane_ref,
    far_a_ref,
    far_b_ref,
    own_halo_ref,
    quart_ref,
    t_ref,
    far_c_ref,
):
    for c in range(3):
        plane_ref[c, 0:NZR, :] = below_ref[c, 0]
        plane_ref[c, NZR : 2 * NZR, :] = pos_ref[c, 0]
        plane_ref[c, 2 * NZR : 3 * NZR, :] = pos_ref[c, 1]
        plane_ref[c, 3 * NZR :, :] = above_ref[c, 0]
    coords = coordinates([plane_ref[c] for c in range(3)], 0.0)
    for ref in (far_a_ref, far_b_ref, far_c_ref):
        empty_ends(ref, S)
    empty_ends(own_halo_ref.at[0], 2 * TERMS)
    empty_ends(own_halo_ref.at[1], 2 * TERMS)
    put_terms(t_ref, far_terms(coords))
    build_far(t_ref, [far_a_ref, None, far_b_ref, far_c_ref])
    put_terms(t_ref, own_terms(coords))
    build_own(t_ref, own_halo_ref, 1)
    zero = jnp.zeros((8, 2 * S), F32)

    def step(z, carry):
        rho, quart = row_sums(z, [far_a_ref, far_b_ref], [0, 2], own_ref, 0, zero, zero)
        rho = rho + sums_ref[pl.ds(z, 1), :]
        quart = quart + sums_ref[pl.ds(NZR + z, 1), :]
        plane_ref[3, pl.ds(NZR + z, 1), :] = rho[:, :S]
        plane_ref[3, pl.ds(2 * NZR + z, 1), :] = rho[:, S:]
        quart_ref[pl.ds(z, 1), :] = quart[:, :S]
        quart_ref[pl.ds(NZR + z, 1), :] = quart[:, S:]
        rho, _ = row_sums(z, [mid_ref, far_c_ref], [1, 3], own_halo_ref, 1, zero, zero)
        plane_ref[3, pl.ds(z, 1), :] = rho[:, :S]
        plane_ref[3, pl.ds(3 * NZR + z, 1), :] = rho[:, S:]
        return carry

    lax.fori_loop(0, NZR, step, 0, unroll=5)


def column(row, rows=S):
    return jnp.broadcast_to(row, (S, S)).T[:rows]


def force_kernel(
    plane_ref,
    low_ref,
    high_ref,
    mid_ref,
    far_a_ref,
    far_b_ref,
    own_ref,
    own_halo_ref,
    quart_ref,
    rank_ref,
    energy_ref,
    forces_ref,
    t_ref,
    rolled_ref,
    far_ref,
    xyz_ref,
    rho_sum_ref,
    quart_sum_ref,
    embed_ref,
    row_ref,
    done_ref,
):
    lane = lax.broadcasted_iota(jnp.int32, (CELLS, S), 1)
    x_low, x_high = low_ref[0], high_ref[0]
    rows_used = jnp.maximum(
        jnp.where((x_low > 0.5) & (x_low < 2.0), S - lane, 0),
        jnp.where(x_high < 0.5, lane + 1, 0),
    )
    needed = jnp.max(rows_used)
    own_pairs = (own_ref, own_halo_ref)
    far0 = (far_a_ref, mid_ref, far_b_ref)
    sides = (rolled_ref, high_ref)
    rho_sum_ref[...] = jnp.zeros(rho_sum_ref.shape, F32)
    quart_sum_ref[...] = jnp.zeros(quart_sum_ref.shape, F32)

    def with_rows(count):
        for c in range(4):
            rolled_ref[c] = low_ref[c] if count == S else pltpu.roll(low_ref[c], count, 1)

        planes = (rolled_ref, plane_ref, high_ref)
        for plane in range(3):
            local = [planes[plane][c] - 0.5 for c in range(3)]
            high = [v.astype(BF16).astype(F32) for v in local]
            rest = [v - h for v, h in zip(local, high)]
            put_terms(
                t_ref, high + [jnp.ones((CELLS, S), F32)] + rest + [jnp.zeros((CELLS, S), F32)]
            )

            def gather(z, carry, plane=plane):
                for kind, (ya, yb) in enumerate(KINDS[:3]):
                    both = jnp.concatenate(
                        [get_terms(t_ref, ya * NZR + z, 8), get_terms(t_ref, yb * NZR + z, 8)], 0
                    )
                    xyz_ref[plane, kind, pl.ds(pl.multiple_of(z * 16, 16), 16), :] = both.astype(BF16)
                return carry

            lax.fori_loop(0, NZR, gather, 0, unroll=2)

        for p in range(2):
            coords = coordinates([sides[p][c] for c in range(3)], (-1.0, 1.0)[p])
            put_terms(t_ref, far_terms(coords))
            build_far(t_ref, [far_ref.at[p, k] for k in range(4)], count)

        def cross(z, carry):
            for p in range(2):
                across = [None] * NYR
                for kind, pairs in USES:
                    rows = far_rows(far_ref.at[p, kind], z + 1, count)
                    total = None
                    for dz in (-1, 0, 1):
                        for pair in pairs:
                            weight = closeness(rows, own_block(own_pairs[pair], z + 1 + dz, kind))
                            square = weight * weight
                            total = square if total is None else total + square
                            at = pl.ds(pl.multiple_of((z + 1 + dz) * 8, 8), 8)
                            rho_sum_ref[pair, at, :] += fold(square)
                            if pair == 0:
                                quart_sum_ref[at, :] += fold(square * square)
                    for half, y in enumerate(KINDS[kind]):
                        part = total[:, half * S : (half + 1) * S]
                        across[y] = part if across[y] is None else across[y] + part
                for y in range(NYR):
                    part = column(sides[p][3, pl.ds(y * NZR + z, 1), :], count)
                    rho = jnp.sum(across[y], 1, keepdims=True) + part
                    at = pl.multiple_of((y * NZR + z) * S, S)
                    embed_ref[2 * p, pl.ds(at, count), :] = 2.5 * lax.rsqrt(rho + 1.0)
            return carry

        lax.fori_loop(0, NZR, cross, 0, unroll=2)

        def finish(z, carry):
            for pair, ys in enumerate(PAIRS):
                at = pl.ds(pl.multiple_of((z + 1) * 8, 8), 8)
                sums = jnp.sum(rho_sum_ref[pair, at, :], 0, keepdims=True)
                for half, y in enumerate(ys):
                    rho = plane_ref[3, pl.ds(y * NZR + z, 1), :] + sums[:, half * S : half * S + S]
                    slope = 2.5 * lax.rsqrt(rho + 1.0)
                    row_ref[pl.ds(y * NZR + z, 1), :] = slope
                    cell_at = pl.multiple_of((y * NZR + z) * S, S)
                    embed_ref[1, pl.ds(cell_at, S), :] = column(slope)
            return carry

        lax.fori_loop(0, NZR, finish, 0, unroll=5)

        def push(i, carry):
            z = i + 1
            rho_at = pl.ds(pl.multiple_of((z + 1) * 8, 8), 8)
            rho_both = jnp.sum(rho_sum_ref[0, rho_at, :], 0, keepdims=True)
            quart_both = jnp.sum(quart_sum_ref[rho_at, :], 0, keepdims=True)
            own = 1.0 + jnp.concatenate(
                [row_ref[pl.ds(NZR + z, 1), :], row_ref[pl.ds(2 * NZR + z, 1), :]], 1
            )
            names = ("all", "x-", "x+", "y-", "y+", "z-", "z+")
            sums = [{n: jnp.zeros((8, S), F32) for n in names} for _ in range(2)]
            for dx in (-1, 0, 1):
                used = S if dx == 0 else count
                for dy in (-1, 0, 1):
                    kind = dy + 1
                    for dz in (-1, 0, 1):
                        if dx == 0:
                            rows = far_rows(far0[kind], z + 1 + dz)
                        else:
                            rows = far_rows(far_ref.at[(dx + 1) // 2, kind], z + 1 + dz, count)
                        weight = closeness(rows, own_block(own_ref, z + 1, kind))
                        slopes = jnp.concatenate(
                            [
                                embed_ref[
                                    dx + 1,
                                    pl.ds(pl.multiple_of((y * NZR + z + dz) * S, S), used),
                                    :,
                                ]
                                for y in KINDS[kind]
                            ],
                            1,
                        )
                        factor = weight * ((own + slopes) - weight * weight)
                        top = factor.astype(BF16)
                        low = (factor - top.astype(F32)).astype(BF16)
                        xyz = xyz_ref[
                            dx + 1, kind, pl.ds(pl.multiple_of((z + dz) * 16, 16), 16), :
                        ][:, :used]
                        both = jnp.dot(xyz, top, preferred_element_type=F32) + jnp.dot(
                            xyz, low, preferred_element_type=F32
                        )
                        keys = ["all"]
                        keys += [a + "-0+"[d + 1] for a, d in zip("xyz", (dx, dy, dz)) if d]
                        for half in range(2):
                            part = both[half * 8 : half * 8 + 8, half * S : half * S + S]
                            for key in keys:
                                sums[half][key] = sums[half][key] + part
            for half in range(2):
                y = half + 1
                at = pl.ds(y * NZR + z, 1)
                occupied = plane_ref[0, at, :] < 2.0
                acc = sums[half]
                weight_sum = acc["all"][3:4]
                rho = plane_ref[3, at, :] + rho_both[:, half * S : (half + 1) * S]
                quart = (
                    quart_ref[pl.ds(half * NZR + z, 1), :]
                    + quart_both[:, half * S : (half + 1) * S]
                )
                results = [-0.2 * jnp.sqrt(rho + 1.0) + 0.01 * (quart - 2.0 * rho)]
                for c, axis in enumerate("xyz"):
                    moved = acc[axis + "+"][3:4] - acc[axis + "-"][3:4]
                    centre = acc["all"][c : c + 1] + acc["all"][c + 4 : c + 5]
                    force = (centre + moved) - (plane_ref[c, at, :] - 0.5) * weight_sum
                    results.append(0.64 * force)
                for k, result in enumerate(results):
                    done_ref[pl.ds(k * OWN + half * 8 + i, 1), :] = jnp.where(
                        occupied, result, 0.0
                    )
            return carry

        lax.fori_loop(0, NZR - 2, push, 0, unroll=2)

    floor = 0
    for count in TIERS:
        pl.when((needed > floor if floor else needed >= 0) & (needed <= count))(
            functools.partial(with_rows, count)
        )
        floor = count

    for k, part in enumerate(split3(done_ref[...])):
        t_ref[k * 4 * OWN : (k + 1) * 4 * OWN, :] = part
    slot = lax.broadcasted_iota(jnp.int32, (S, S), 0).astype(F32)
    for cell in range(OWN):
        chosen = jnp.where(slot == rank_ref[cell : cell + 1, :], 1.0, 0.0).astype(BF16)
        rows = t_ref[pl.ds(cell, 16, stride=OWN), :].astype(BF16)
        moved = jnp.dot(rows, chosen, preferred_element_type=F32)
        moved = (moved[0:4] + moved[4:8]) + moved[8:12]
        energy_ref[cell : cell + 1, :] = moved[0:1]
        for c in range(3):
            forces_ref[c * OWN + cell : c * OWN + cell + 1, :] = moved[c + 1 : c + 2]


def ring(axis, step):
    count = lax.axis_size(axis)
    return [(i, (i + step) % count) for i in range(count)]


def kernel_call(body, outs, scratch, name, **specs):
    return pl.pallas_call(
        body,
        **specs,
        out_shape=tuple(jax.ShapeDtypeStruct(shape, dtype) for shape, dtype in outs),
        scratch_shapes=[pltpu.VMEM(*s) if isinstance(s, tuple) else s for s in scratch],
        compiler_params=pltpu.CompilerParams(vmem_limit_bytes=VMEM_LIMIT),
        name=name,
    )


FAR = ((SLOTS * S, 2 * TERMS), BF16)
OWN_BLOCKS = ((2, SLOTS * 2 * TERMS, 2 * S), BF16)
TERM_ROWS = ((TERMS * CELLS, S), F32)


def sort_cells(positions, counts):
    return kernel_call(
        sort_kernel,
        [((3, OWN, S), F32), ((OWN, S), F32)],
        [
            ((16 * OWN, S), F32),
            ((3, 1, 2, 8, S), F32),
            pltpu.SMEM((1, 2, 8), jnp.int32),
            pltpu.SemaphoreType.DMA(()),
            pltpu.SemaphoreType.DMA(()),
        ],
        "sort",
        in_specs=[pl.BlockSpec(memory_space=pltpu.HBM)] * 2,
    )(positions, counts)


def pair_row(rows):
    return kernel_call(
        pair_row_kernel,
        [FAR, OWN_BLOCKS, ((2 * NZR, 2 * S), F32)],
        [TERM_ROWS, ((3, CELLS, S), F32)],
        "rows",
    )(rows)


def plane_sums(rows, below, above, mid, own, sums):
    return kernel_call(
        plane_kernel,
        [((4, CELLS, S), F32), FAR, FAR, OWN_BLOCKS, ((2 * NZR, S), F32)],
        [TERM_ROWS, FAR],
        "plane",
    )(rows, below, above, mid, own, sums)


def finish_forces(*operands):
    return kernel_call(
        force_kernel,
        [((OWN, S), F32), ((3 * OWN, S), F32)],
        [
            TERM_ROWS,
            ((4, CELLS, S), F32),
            ((2, 4, SLOTS * S, 2 * TERMS), BF16),
            ((3, 3, NZR * 16, S), BF16),
            ((2, SLOTS * 8, 2 * S), F32),
            ((SLOTS * 8, 2 * S), F32),
            ((3, CELLS * S, S), F32),
            ((CELLS, S), F32),
            ((4 * OWN, S), F32),
        ],
        "forces",
    )(*operands)


def per_device(positions, counts):
    positions = pltpu.with_memory_space_constraint(positions, pltpu.HBM)
    counts = pltpu.with_memory_space_constraint(counts, pltpu.HBM)
    sorted_own, rank = sort_cells(positions, counts)
    cells = sorted_own.reshape(3, 2, 8, S)
    behind = lax.ppermute(cells[:, :, 7:8], "gz", ring("gz", 1))
    ahead = lax.ppermute(cells[:, :, 0:1], "gz", ring("gz", -1))
    rows = jnp.concatenate([behind, cells, ahead], axis=2)
    below = lax.ppermute(rows[:, 1:2], "gy", ring("gy", 1))
    above = lax.ppermute(rows[:, 0:1], "gy", ring("gy", -1))
    mid, own, sums = pair_row(rows)
    plane, far_a, far_b, own_halo, quart = plane_sums(rows, below, above, mid, own, sums)
    low = lax.ppermute(plane, "gx", ring("gx", 1))
    high = lax.ppermute(plane, "gx", ring("gx", -1))
    energy, forces = finish_forces(
        plane, low, high, mid, far_a, far_b, own, own_halo, quart, rank
    )
    return (energy.reshape(1, 2, 8, S), forces.reshape(3, 1, 2, 8, S))


def solution(mesh):
    placed = (P(None, "gx", "gy", "gz", None), P("gx", "gy", "gz"))
    return jax.shard_map(
        per_device,
        mesh=mesh,
        in_specs=placed,
        out_specs=(P("gx", "gy", "gz", None), P(None, "gx", "gy", "gz", None)),
        check_vma=False,
    )
```

```python
import functools

import jax
import jax.numpy as jnp
from jax import lax
from jax.experimental import pallas as pl
from jax.experimental.pallas import tpu as pltpu
from jax.sharding import PartitionSpec as P

SENTINEL = 4.0
S = 128
NYR = 4
NZR = 10
CELLS = NYR * NZR
SLOTS = NZR + 2
TERMS = 32
KINDS = ((0, 1), (1, 2), (2, 3), (0, 3))
PAIRS = ((1, 2), (0, 3))
USES = ((0, (0,)), (1, (0, 1)), (2, (0,)), (3, (1,)))
TIERS = (80, 96, S)
OWN = 16
VMEM_LIMIT = 24 * 2**20
F32 = jnp.float32
BF16 = jnp.bfloat16


def split3(value):
    high = value.astype(BF16).astype(F32)
    rest = value - high
    mid = rest.astype(BF16).astype(F32)
    return high, mid, rest - mid


def coordinates(comps, plane):
    rows = lax.broadcasted_iota(jnp.int32, (CELLS, S), 0)
    y_row = (
        (rows >= NZR).astype(jnp.int32)
        + (rows >= 2 * NZR).astype(jnp.int32)
        + (rows >= 3 * NZR).astype(jnp.int32)
    )
    z_row = rows - NZR * y_row
    return (
        comps[0] + (plane - 0.5),
        comps[1] + (y_row.astype(F32) - 2.0),
        comps[2] + (z_row.astype(F32) - 5.0),
    )


def put_terms(t_ref, terms):
    for k, term in enumerate(terms):
        t_ref[k * CELLS : (k + 1) * CELLS, :] = term


def get_terms(t_ref, cell, count):
    return t_ref[pl.ds(cell, count, stride=CELLS), :]


def far_terms(coords):
    one = jnp.ones((CELLS, S), F32)
    zero = jnp.zeros((CELLS, S), F32)
    out = []
    for c in coords:
        h, m, l = split3(c)
        out += [h, h, h, m, m, l]
    norm = coords[0] * coords[0] + coords[1] * coords[1] + coords[2] * coords[2]
    return out + [one, one, one] + list(split3(-4.0 * norm)) + [zero] * 8


def own_terms(coords):
    one = jnp.ones((CELLS, S), F32)
    zero = jnp.zeros((CELLS, S), F32)
    out = []
    for c in coords:
        h, m, l = split3(8.0 * c)
        out += [h, m, l, h, m, h]
    norm = coords[0] * coords[0] + coords[1] * coords[1] + coords[2] * coords[2]
    return out + list(split3(1.0 - 4.0 * norm)) + [one, one, one] + [zero] * 8


def build_far(t_ref, far_refs, rows=S):
    low_half = lax.broadcasted_iota(jnp.int32, (rows, 2 * TERMS), 1) < TERMS

    def step(z, carry):
        sides = []
        for y in (0, 2):
            both = jnp.concatenate(
                [get_terms(t_ref, y * NZR + z, TERMS), get_terms(t_ref, (y + 1) * NZR + z, TERMS)],
                0,
            )
            sides.append(both.T[:rows])
        at = pl.multiple_of((z + 1) * S, S)
        for far_ref, first, second in zip(far_refs, (0, 1, 1, 0), (0, 0, 1, 1)):
            if far_ref is None:
                continue
            value = sides[first]
            if first != second:
                value = jnp.where(low_half, sides[first], sides[second])
            far_ref[pl.ds(at, rows), :] = value.astype(BF16)
        return carry

    lax.fori_loop(0, NZR, step, 0, unroll=5)


def build_own(t_ref, own_ref, pair):
    zero = jnp.zeros((TERMS, S), F32)
    ya, yb = PAIRS[pair]

    def step(z, carry):
        a = get_terms(t_ref, ya * NZR + z, TERMS)
        b = get_terms(t_ref, yb * NZR + z, TERMS)
        a = jnp.concatenate([a, zero], 1).astype(BF16)
        b = jnp.concatenate([zero, b], 1).astype(BF16)
        at = pl.multiple_of((z + 1) * 2 * TERMS, 2 * TERMS)
        own_ref[0, pl.ds(at, 2 * TERMS), :] = jnp.concatenate([a, b], 0)
        own_ref[1, pl.ds(at, 2 * TERMS), :] = jnp.concatenate([b, a], 0)
        return carry

    lax.fori_loop(0, NZR, step, 0, unroll=5)


def empty_ends(ref, size):
    for slot in (0, SLOTS - 1):
        ref[slot * size : (slot + 1) * size, :] = jnp.zeros((size, ref.shape[1]), BF16)


def fold(value):
    return jnp.sum(value.reshape(value.shape[0] // 8, 8, value.shape[-1]), axis=0)


def far_rows(far_ref, slot, rows=S):
    return far_ref[pl.ds(pl.multiple_of(slot * S, S), rows), :]


def own_block(own_ref, slot, kind):
    at = pl.multiple_of(slot * 2 * TERMS, 2 * TERMS)
    return own_ref[1 if kind == 1 else 0, pl.ds(at, 2 * TERMS), :]


def closeness(rows, block):
    return jnp.maximum(jnp.dot(rows, block, preferred_element_type=F32), 0.0)


def sort_kernel(pos_hbm, counts_hbm, own_ref, rank_ref, t_ref, pos_ref, counts_ref, sem_p, sem_c):
    copy_p = pltpu.make_async_copy(pos_hbm, pos_ref, sem_p)
    copy_c = pltpu.make_async_copy(counts_hbm, counts_ref, sem_c)
    copy_p.start()
    copy_c.start()
    copy_p.wait()
    copy_c.wait()
    lane = lax.broadcasted_iota(jnp.int32, (OWN, S), 1)
    row = lax.broadcasted_iota(jnp.int32, (OWN, S), 0)
    held = jnp.zeros((OWN, S), jnp.int32)
    for cell in range(OWN):
        held = jnp.where(row == cell, counts_ref[0, cell // 8, cell % 8], held)
    occupied = lane < held
    comps = [
        jnp.where(occupied, jnp.concatenate([pos_ref[c, 0, 0], pos_ref[c, 0, 1]], 0), SENTINEL)
        for c in range(3)
    ]
    low = occupied & (comps[0] < 0.5)
    high = occupied & (comps[0] >= 0.5)
    up_to = lax.broadcasted_iota(jnp.int32, (S, S), 0) <= lax.broadcasted_iota(
        jnp.int32, (S, S), 1
    )
    up_to = jnp.where(up_to, 1.0, 0.0).astype(BF16)
    flags = jnp.concatenate([jnp.where(m, 1.0, 0.0) for m in (low, high, ~occupied)], 0)
    before = jnp.dot(flags.astype(BF16), up_to, preferred_element_type=F32)
    lows, highs, blanks = before[:OWN], before[OWN : 2 * OWN], before[2 * OWN :]
    all_low = jnp.max(lows, axis=1, keepdims=True)
    rank = jnp.where(low, lows - 1.0, jnp.where(high, S - highs, all_low + blanks - 1.0))
    rank_ref[...] = rank
    terms = []
    for c in comps:
        terms += list(split3(c))
    for k, term in enumerate(terms + [jnp.zeros((OWN, S), F32)] * 7):
        t_ref[k * OWN : (k + 1) * OWN, :] = term
    slot = lax.broadcasted_iota(jnp.int32, (S, S), 0).astype(F32)
    for cell in range(OWN):
        chosen = jnp.where(slot == rank[cell : cell + 1], 1.0, 0.0).astype(BF16)
        rows = t_ref[pl.ds(cell, 16, stride=OWN), :].astype(BF16)
        moved = lax.dot_general(
            rows, chosen, (((1,), (1,)), ((), ())), preferred_element_type=F32
        )
        for c in range(3):
            own_ref[c, cell : cell + 1, :] = (
                moved[3 * c : 3 * c + 1] + moved[3 * c + 1 : 3 * c + 2]
            ) + moved[3 * c + 2 : 3 * c + 3]


def itself():
    row = lax.broadcasted_iota(jnp.int32, (S, 2 * S), 0)
    lane = lax.broadcasted_iota(jnp.int32, (S, 2 * S), 1)
    return (row == lane) | (row + S == lane)


def row_sums(z, far_refs, kinds, own_ref, pair):
    rho = jnp.zeros((8, 2 * S), F32)
    for kind, far_ref in zip(kinds, far_refs):
        for dz in (-1, 0, 1):
            weight = closeness(far_rows(far_ref, z + 1 + dz), own_block(own_ref, z + 1, kind))
            square = weight * weight
            if dz == 0 and KINDS[kind] == PAIRS[pair]:
                square = jnp.where(itself(), 0.0, square)
            rho = rho + fold(square)
    return jnp.sum(rho, 0, keepdims=True)


def put_gathered(t_ref, xyz_refs, terms):
    put_terms(t_ref, terms)

    def gather(z, carry):
        for kind, (ya, yb) in enumerate(KINDS[:3]):
            both = jnp.concatenate(
                [get_terms(t_ref, ya * NZR + z, 8), get_terms(t_ref, yb * NZR + z, 8)], 0
            )
            xyz_refs[kind, pl.ds(pl.multiple_of(z * 16, 16), 16), :] = both.astype(BF16)
        return carry

    lax.fori_loop(0, NZR, gather, 0, unroll=5)


def split2(value):
    high = value.astype(BF16)
    return high, (value - high.astype(F32)).astype(BF16)


def local_terms(comps):
    local = [c - 0.5 for c in comps]
    high = [v.astype(BF16).astype(F32) for v in local]
    rest = [v - h for v, h in zip(local, high)]
    return high + [jnp.ones((CELLS, S), F32)] + rest + [jnp.zeros((CELLS, S), F32)]


def no_sums():
    names = ("all", "x-", "x+", "y-", "y+", "z-", "z+")
    return [{n: jnp.zeros((8, S), F32) for n in names} for _ in range(2)]


def add_sums(sums, rows, limbs, offset):
    both = sum(jnp.dot(rows, limb, preferred_element_type=F32) for limb in limbs)
    keys = ["all"] + [a + "-0+"[d + 1] for a, d in zip("xyz", offset) if d]
    for part_of, held in enumerate(sums):
        for half in range(2):
            at = part_of * 16 + half * 8
            part = both[at : at + 8, half * S : half * S + S]
            for key in keys:
                held[half][key] = held[half][key] + part


def resolve(acc):
    both = {key: value[0:4] + value[4:8] for key, value in acc.items()}
    out = [
        both["all"][c : c + 1] + (both[a + "+"][3:4] - both[a + "-"][3:4])
        for c, a in enumerate("xyz")
    ]
    return out + [both["all"][3:4]]


def pair_row_kernel(pos_ref, far_ref, own_ref, sums_ref, t_ref, whole_ref):
    for c in range(3):
        for y in range(2):
            whole_ref[c, (y + 1) * NZR : (y + 2) * NZR, :] = pos_ref[c, y]
            whole_ref[c, y * 3 * NZR : (y * 3 + 1) * NZR, :] = jnp.zeros((NZR, S), F32)
    coords = coordinates([whole_ref[c] for c in range(3)], 0.0)
    empty_ends(far_ref, S)
    empty_ends(own_ref.at[0], 2 * TERMS)
    empty_ends(own_ref.at[1], 2 * TERMS)
    put_terms(t_ref, far_terms(coords))
    build_far(t_ref, [None, far_ref, None, None])
    put_terms(t_ref, own_terms(coords))
    build_own(t_ref, own_ref, 0)

    def step(z, carry):
        sums_ref[pl.ds(z, 1), :] = row_sums(z, [far_ref], [1], own_ref, 0)
        return carry

    lax.fori_loop(0, NZR, step, 0, unroll=5)


def plane_kernel(
    pos_ref,
    below_ref,
    above_ref,
    mid_ref,
    own_ref,
    sums_ref,
    plane_ref,
    far_a_ref,
    far_b_ref,
    own_halo_ref,
    t_ref,
    far_c_ref,
):
    for c in range(3):
        plane_ref[c, 0:NZR, :] = below_ref[c, 0]
        plane_ref[c, NZR : 2 * NZR, :] = pos_ref[c, 0]
        plane_ref[c, 2 * NZR : 3 * NZR, :] = pos_ref[c, 1]
        plane_ref[c, 3 * NZR :, :] = above_ref[c, 0]
    coords = coordinates([plane_ref[c] for c in range(3)], 0.0)
    for ref in (far_a_ref, far_b_ref, far_c_ref):
        empty_ends(ref, S)
    empty_ends(own_halo_ref.at[0], 2 * TERMS)
    empty_ends(own_halo_ref.at[1], 2 * TERMS)
    put_terms(t_ref, far_terms(coords))
    build_far(t_ref, [far_a_ref, None, far_b_ref, far_c_ref])
    put_terms(t_ref, own_terms(coords))
    build_own(t_ref, own_halo_ref, 1)

    def step(z, carry):
        rho = row_sums(z, [far_a_ref, far_b_ref], [0, 2], own_ref, 0) + sums_ref[pl.ds(z, 1), :]
        plane_ref[3, pl.ds(NZR + z, 1), :] = rho[:, :S]
        plane_ref[3, pl.ds(2 * NZR + z, 1), :] = rho[:, S:]
        rho = row_sums(z, [mid_ref, far_c_ref], [1, 3], own_halo_ref, 1)
        plane_ref[3, pl.ds(z, 1), :] = rho[:, :S]
        plane_ref[3, pl.ds(3 * NZR + z, 1), :] = rho[:, S:]
        return carry

    lax.fori_loop(0, NZR, step, 0, unroll=5)


def inner_kernel(
    plane_ref,
    mid_ref,
    far_a_ref,
    far_b_ref,
    own_ref,
    top_ref,
    low_ref,
    cube_ref,
    quart_ref,
    xyz_ref,
    t_ref,
):
    far0 = (far_a_ref, mid_ref, far_b_ref)
    put_gathered(t_ref, xyz_ref, local_terms([plane_ref[c] for c in range(3)]))

    def step(i, carry):
        z = i + 1
        cube = no_sums()
        quart = jnp.zeros((8, 2 * S), F32)
        for kind in range(3):
            for dz in (-1, 0, 1):
                weight = closeness(
                    far_rows(far0[kind], z + 1 + dz), own_block(own_ref, z + 1, kind)
                )
                if kind == 1 and dz == 0:
                    weight = jnp.where(itself(), 0.0, weight)
                square = weight * weight
                quart = quart + fold(square * square)
                limbs = split2(weight)
                at = pl.ds(pl.multiple_of((i * 9 + kind * 3 + dz + 1) * S, S), S)
                top_ref[at, :] = limbs[0]
                low_ref[at, :] = limbs[1]
                rows = xyz_ref[kind, pl.ds(pl.multiple_of((z + dz) * 16, 16), 16), :]
                add_sums([cube], rows, split2(square * weight), (0, kind - 1, dz))
        quart = jnp.sum(quart, 0, keepdims=True)
        for half in range(2):
            for c, part in enumerate(resolve(cube[half])):
                cube_ref[pl.ds((half * 4 + c) * 8 + i, 1), :] = part
            quart_ref[pl.ds(half * 8 + i, 1), :] = quart[:, half * S : (half + 1) * S]
        return carry

    lax.fori_loop(0, NZR - 2, step, 0, unroll=2)


def column(row, rows=S):
    return jnp.broadcast_to(row, (S, S)).T[:rows]


def force_kernel(
    plane_ref,
    low_ref,
    high_ref,
    own_ref,
    own_halo_ref,
    top_ref,
    rest_ref,
    cube_ref,
    quart_ref,
    local_ref,
    rank_ref,
    energy_ref,
    forces_ref,
    t_ref,
    rolled_ref,
    far_ref,
    xyz_ref,
    rho_sum_ref,
    quart_sum_ref,
    embed_ref,
    row_ref,
    done_ref,
):
    lane = lax.broadcasted_iota(jnp.int32, (CELLS, S), 1)
    x_low, x_high = low_ref[0], high_ref[0]
    rows_used = jnp.maximum(
        jnp.where((x_low > 0.5) & (x_low < 2.0), S - lane, 0),
        jnp.where(x_high < 0.5, lane + 1, 0),
    )
    needed = jnp.max(rows_used)
    own_pairs = (own_ref, own_halo_ref)
    sides = (rolled_ref, high_ref)
    rho_sum_ref[...] = jnp.zeros(rho_sum_ref.shape, F32)
    quart_sum_ref[...] = jnp.zeros(quart_sum_ref.shape, F32)

    def with_rows(count):
        for c in range(4):
            rolled_ref[c] = low_ref[c] if count == S else pltpu.roll(low_ref[c], count, 1)

        for p in range(2):
            put_gathered(t_ref, xyz_ref.at[2 * p], local_terms([sides[p][c] for c in range(3)]))

        for p in range(2):
            coords = coordinates([sides[p][c] for c in range(3)], (-1.0, 1.0)[p])
            put_terms(t_ref, far_terms(coords))
            build_far(t_ref, [far_ref.at[p, k] for k in range(4)], count)

        def cross(z, carry):
            for p in range(2):
                across = [None] * NYR
                for kind, pairs in USES:
                    rows = far_rows(far_ref.at[p, kind], z + 1, count)
                    total = None
                    for dz in (-1, 0, 1):
                        for pair in pairs:
                            weight = closeness(rows, own_block(own_pairs[pair], z + 1 + dz, kind))
                            square = weight * weight
                            total = square if total is None else total + square
                            at = pl.ds(pl.multiple_of((z + 1 + dz) * 8, 8), 8)
                            rho_sum_ref[pair, at, :] += fold(square)
                            if pair == 0:
                                quart_sum_ref[at, :] += fold(square * square)
                    for half, y in enumerate(KINDS[kind]):
                        part = total[:, half * S : (half + 1) * S]
                        across[y] = part if across[y] is None else across[y] + part
                for y in range(NYR):
                    part = column(sides[p][3, pl.ds(y * NZR + z, 1), :], count)
                    rho = jnp.sum(across[y], 1, keepdims=True) + part
                    at = pl.multiple_of((y * NZR + z) * S, S)
                    embed_ref[p, pl.ds(at, count), :] = 2.5 * lax.rsqrt(rho + 1.0)
            return carry

        lax.fori_loop(0, NZR, cross, 0, unroll=5)

        def finish(z, carry):
            for pair, ys in enumerate(PAIRS):
                at = pl.ds(pl.multiple_of((z + 1) * 8, 8), 8)
                sums = jnp.sum(rho_sum_ref[pair, at, :], 0, keepdims=True)
                for half, y in enumerate(ys):
                    rho = plane_ref[3, pl.ds(y * NZR + z, 1), :] + sums[:, half * S : half * S + S]
                    row_ref[pl.ds(y * NZR + z, 1), :] = 2.5 * lax.rsqrt(rho + 1.0)
            return carry

        lax.fori_loop(0, NZR, finish, 0, unroll=5)
        slopes = row_ref[...]
        weighted = [slopes * (plane_ref[c] - 0.5) for c in range(3)] + [slopes]
        high = [v.astype(BF16).astype(F32) for v in weighted]
        put_gathered(t_ref, xyz_ref.at[1], high + [v - h for v, h in zip(weighted, high)])

        def push(i, carry):
            z = i + 1
            rho_at = pl.ds(pl.multiple_of((z + 1) * 8, 8), 8)
            rho_both = jnp.sum(rho_sum_ref[0, rho_at, :], 0, keepdims=True)
            quart_both = jnp.sum(quart_sum_ref[rho_at, :], 0, keepdims=True)
            own = 1.0 + jnp.concatenate(
                [row_ref[pl.ds(NZR + z, 1), :], row_ref[pl.ds(2 * NZR + z, 1), :]], 1
            )
            sums, line = no_sums(), no_sums()
            for dx in (0, -1, 1):
                for kind in range(3):
                    for dz in (-1, 0, 1):
                        xyz = xyz_ref[
                            dx + 1, kind, pl.ds(pl.multiple_of((z + dz) * 16, 16), 16), :
                        ]
                        offset = (dx, kind - 1, dz)
                        if dx == 0:
                            at = pl.ds(pl.multiple_of((i * 9 + kind * 3 + dz + 1) * S, S), S)
                            local = local_ref[
                                kind, pl.ds(pl.multiple_of((z + dz) * 16, 16), 16), :
                            ]
                            add_sums(
                                [sums, line],
                                jnp.concatenate([xyz, local], 0),
                                (top_ref[at, :], rest_ref[at, :]),
                                offset,
                            )
                            continue
                        rows = far_rows(far_ref.at[(dx + 1) // 2, kind], z + 1 + dz, count)
                        weight = closeness(rows, own_block(own_ref, z + 1, kind))
                        slopes = jnp.concatenate(
                            [
                                embed_ref[
                                    (dx + 1) // 2,
                                    pl.ds(pl.multiple_of((y * NZR + z + dz) * S, S), count),
                                    :,
                                ]
                                for y in KINDS[kind]
                            ],
                            1,
                        )
                        factor = weight * ((own + slopes) - weight * weight)
                        add_sums([sums], xyz[:, :count], split2(factor), offset)
            for half in range(2):
                y = half + 1
                at = pl.ds(y * NZR + z, 1)
                occupied = plane_ref[0, at, :] < 2.0
                lanes = slice(half * S, (half + 1) * S)
                moved = []
                for c, (part, first) in enumerate(zip(resolve(sums[half]), resolve(line[half]))):
                    cube = cube_ref[pl.ds((half * 4 + c) * 8 + i, 1), :]
                    moved.append(part + (own[:, lanes] * first - cube))
                rho = plane_ref[3, at, :] + rho_both[:, lanes]
                quart = quart_ref[pl.ds(half * 8 + i, 1), :] + quart_both[:, lanes]
                results = [-0.2 * jnp.sqrt(rho + 1.0) + 0.01 * (quart - 2.0 * rho)]
                for c in range(3):
                    force = moved[c] - (plane_ref[c, at, :] - 0.5) * moved[3]
                    results.append(0.64 * force)
                for k, result in enumerate(results):
                    done_ref[pl.ds(k * OWN + half * 8 + i, 1), :] = jnp.where(
                        occupied, result, 0.0
                    )
            return carry

        lax.fori_loop(0, NZR - 2, push, 0, unroll=2)

    floor = 0
    for count in TIERS:
        pl.when((needed > floor if floor else needed >= 0) & (needed <= count))(
            functools.partial(with_rows, count)
        )
        floor = count

    for k, part in enumerate(split3(done_ref[...])):
        t_ref[k * 4 * OWN : (k + 1) * 4 * OWN, :] = part
    slot = lax.broadcasted_iota(jnp.int32, (S, S), 0).astype(F32)
    for cell in range(OWN):
        chosen = jnp.where(slot == rank_ref[cell : cell + 1, :], 1.0, 0.0).astype(BF16)
        rows = t_ref[pl.ds(cell, 16, stride=OWN), :].astype(BF16)
        moved = jnp.dot(rows, chosen, preferred_element_type=F32)
        moved = (moved[0:4] + moved[4:8]) + moved[8:12]
        energy_ref[cell : cell + 1, :] = moved[0:1]
        for c in range(3):
            forces_ref[c * OWN + cell : c * OWN + cell + 1, :] = moved[c + 1 : c + 2]


def ring(axis, step):
    count = lax.axis_size(axis)
    return [(i, (i + step) % count) for i in range(count)]


def kernel_call(body, outs, scratch, name, **specs):
    return pl.pallas_call(
        body,
        **specs,
        out_shape=tuple(jax.ShapeDtypeStruct(shape, dtype) for shape, dtype in outs),
        scratch_shapes=[pltpu.VMEM(*s) if isinstance(s, tuple) else s for s in scratch],
        compiler_params=pltpu.CompilerParams(vmem_limit_bytes=VMEM_LIMIT),
        name=name,
    )


FAR = ((SLOTS * S, 2 * TERMS), BF16)
OWN_BLOCKS = ((2, SLOTS * 2 * TERMS, 2 * S), BF16)
TERM_ROWS = ((TERMS * CELLS, S), F32)


def sort_cells(positions, counts):
    return kernel_call(
        sort_kernel,
        [((3, OWN, S), F32), ((OWN, S), F32)],
        [
            ((16 * OWN, S), F32),
            ((3, 1, 2, 8, S), F32),
            pltpu.SMEM((1, 2, 8), jnp.int32),
            pltpu.SemaphoreType.DMA(()),
            pltpu.SemaphoreType.DMA(()),
        ],
        "sort",
        in_specs=[pl.BlockSpec(memory_space=pltpu.HBM)] * 2,
    )(positions, counts)


def pair_row(rows):
    return kernel_call(
        pair_row_kernel,
        [FAR, OWN_BLOCKS, ((NZR, 2 * S), F32)],
        [TERM_ROWS, ((3, CELLS, S), F32)],
        "rows",
    )(rows)


def plane_sums(rows, below, above, mid, own, sums):
    return kernel_call(
        plane_kernel,
        [((4, CELLS, S), F32), FAR, FAR, OWN_BLOCKS],
        [TERM_ROWS, FAR],
        "plane",
    )(rows, below, above, mid, own, sums)


def inner_sums(*operands):
    return kernel_call(
        inner_kernel,
        [
            ((8 * 9 * S, 2 * S), BF16),
            ((8 * 9 * S, 2 * S), BF16),
            ((8 * 8, S), F32),
            ((OWN, S), F32),
            ((3, NZR * 16, S), BF16),
        ],
        [TERM_ROWS],
        "inner",
    )(*operands)


def finish_forces(*operands):
    return kernel_call(
        force_kernel,
        [((OWN, S), F32), ((3 * OWN, S), F32)],
        [
            TERM_ROWS,
            ((4, CELLS, S), F32),
            ((2, 4, SLOTS * S, 2 * TERMS), BF16),
            ((3, 3, NZR * 16, S), BF16),
            ((2, SLOTS * 8, 2 * S), F32),
            ((SLOTS * 8, 2 * S), F32),
            ((2, CELLS * S, S), F32),
            ((CELLS, S), F32),
            ((4 * OWN, S), F32),
        ],
        "forces",
    )(*operands)


def per_device(positions, counts):
    positions = pltpu.with_memory_space_constraint(positions, pltpu.HBM)
    counts = pltpu.with_memory_space_constraint(counts, pltpu.HBM)
    sorted_own, rank = sort_cells(positions, counts)
    cells = sorted_own.reshape(3, 2, 8, S)
    behind = lax.ppermute(cells[:, :, 7:8], "gz", ring("gz", 1))
    ahead = lax.ppermute(cells[:, :, 0:1], "gz", ring("gz", -1))
    rows = jnp.concatenate([behind, cells, ahead], axis=2)
    below = lax.ppermute(rows[:, 1:2], "gy", ring("gy", 1))
    above = lax.ppermute(rows[:, 0:1], "gy", ring("gy", -1))
    mid, own, sums = pair_row(rows)
    plane, far_a, far_b, own_halo = plane_sums(rows, below, above, mid, own, sums)
    low = lax.ppermute(plane, "gx", ring("gx", 1))
    high = lax.ppermute(plane, "gx", ring("gx", -1))
    inner = inner_sums(plane, mid, far_a, far_b, own)
    energy, forces = finish_forces(plane, low, high, own, own_halo, *inner, rank)
    return (energy.reshape(1, 2, 8, S), forces.reshape(3, 1, 2, 8, S))


def solution(mesh):
    placed = (P(None, "gx", "gy", "gz", None), P("gx", "gy", "gz"))
    return jax.shard_map(
        per_device,
        mesh=mesh,
        in_specs=placed,
        out_specs=(P("gx", "gy", "gz", None), P(None, "gx", "gy", "gz", None)),
        check_vma=False,
    )
```
